32 devices in a mesh: dp: 4 (over z), mp: 8 (over y, x, core).
Axes of the slice: x: 2, y: 2, z: 4, core: 2. Of those that a mesh axis runs over, the one named last changes fastest.
Arguments:
- policy_hidden: bfloat16 [256, 3584], P('dp'), may hold values from -96 to 96
- reference_hidden: bfloat16 [256, 3584], P('dp'), may hold values from -96 to 96
- policy_gain: float32 [3584], replicated, may hold values from 0.5 to 1.5
- reference_gain: float32 [3584], replicated, may hold values from 0.5 to 1.5
- policy_embedding: bfloat16 [131072, 3584], P(('dp', 'mp')), may hold values from -1 to 1
- reference_embedding: bfloat16 [131072, 3584], P(('dp', 'mp')), may hold values from -1 to 1
- mixture_weight: float32 [256], replicated, may hold values from 0.1 to 0.9
- sampled_tokens: int32 [256], replicated, may hold values from 0 to 131071
Outputs:
- mixture_shift: float32 [256, 131072], P(None, ('dp', 'mp'))
- sampled_logprobs: float32 [3, 256], P(None, 'dp')
The draws below stay inside these ranges and needn't reach their ends.
All inputs are finite; a program needn't handle non-finite values.
Results may differ from the reference program's by a relative error of at most 0.002.
Values may be sent and summed in bfloat16 or wider, within the bound.
A program may use at most 128 MiB of HBM per device.

```python
import math
import jax
import jax.numpy as jnp
from jax import lax

D = 3584
VOCAB = 131072
BATCH = 256


def hidden_states(key):
    keys = jax.random.split(key, 3)
    rows = jnp.exp(jax.random.uniform(keys[1], (BATCH, 1), jnp.float32, 0.0, math.log(10.0)))
    columns = jnp.exp(jax.random.uniform(keys[2], (1, D), jnp.float32, -1.15, 1.15))
    base = jax.random.normal(keys[0], (BATCH, D), jnp.float32)
    return jnp.clip(base * rows * columns, -96.0, 96.0).astype(jnp.bfloat16)


def embedding_rows(key):
    keys = jax.random.split(key, 2)
    place = jnp.arange(VOCAB, dtype=jnp.float32)[:, None] / VOCAB
    jitter = jnp.exp(jax.random.uniform(keys[1], (VOCAB, 1), jnp.float32, -0.5, 0.5))
    scale = 4.0 / math.sqrt(D) * (0.6 + 1.2 * place) * jitter
    base = jax.random.normal(keys[0], (VOCAB, D), jnp.float32)
    return jnp.clip(base * scale, -1.0, 1.0).astype(jnp.bfloat16)


def draw_policy_hidden(key, part):
    return hidden_states(jax.random.fold_in(key, 11))


def draw_reference_hidden(key, part):
    return hidden_states(jax.random.fold_in(key, 12))


def draw_policy_embedding(key, part):
    return embedding_rows(jax.random.fold_in(key, 21))


def draw_reference_embedding(key, part):
    return embedding_rows(jax.random.fold_in(key, 22))


def plant(array, own_key, least, high):
    extent = array.shape
    index_at = [jax.random.randint(jax.random.fold_in(own_key, axis), (), 0, extent[axis]) for axis in range(len(extent))]
    array = array.at[tuple(index_at)].set(least)
    longest = extent.index(max(extent))
    index_at[longest] = (index_at[longest] + 1) % extent[longest]
    return array.at[tuple(index_at)].set(high)


def setup_inputs(seed: int = 0) -> dict:
    key_of = jax.random.split(jax.random.key(seed), 9)
    return {
        "policy_hidden": draw_policy_hidden(jax.random.fold_in(key_of[8], 71), 0),
        "reference_hidden": draw_reference_hidden(jax.random.fold_in(key_of[8], 71), 0),
        "policy_gain": jnp.clip(1.0 + 0.1 * jax.random.normal(key_of[2], (D,), jnp.float32), 0.5, 1.5),
        "reference_gain": jnp.clip(1.0 + 0.1 * jax.random.normal(key_of[3], (D,), jnp.float32), 0.5, 1.5),
        "policy_embedding": draw_policy_embedding(jax.random.fold_in(key_of[8], 71), 0),
        "reference_embedding": draw_reference_embedding(jax.random.fold_in(key_of[8], 71), 0),
        "mixture_weight": jnp.clip(jax.random.uniform(key_of[6], (BATCH,), jnp.float32, 0.1, 0.9), 0.1, 0.9),
        "sampled_tokens": plant(jax.random.randint(key_of[7], (BATCH,), 0, VOCAB), jax.random.fold_in(key_of[7], 1), 0, VOCAB - 1).astype(jnp.int32),
    }


softcap = 30.0
epsilon = 1e-06

def normalize(hidden, gain):
    values = hidden.astype(jnp.float32)
    meansq = lax.optimization_barrier(jnp.mean(values * values, axis=-1, keepdims=True))
    return (values * lax.rsqrt(meansq + epsilon) * gain).astype(jnp.bfloat16)

def project(normed, embedding):
    raw = lax.dot_general(normed, embedding, (((1,), (1,)), ((), ())), preferred_element_type=jnp.float32)
    return softcap * jnp.tanh(raw / softcap)

def reference(policy_hidden, reference_hidden, policy_gain, reference_gain, policy_embedding, reference_embedding, mixture_weight, sampled_tokens):
    capped_policy = project(normalize(policy_hidden, policy_gain), policy_embedding)
    capped_reference = project(normalize(reference_hidden, reference_gain), reference_embedding)
    weight = mixture_weight[:, None]
    mixed = (1.0 - weight) * capped_policy + weight * capped_reference
    policy_total = jnp.log(lax.optimization_barrier(jnp.sum(jnp.exp(capped_policy), axis=1)))
    reference_total = jnp.log(lax.optimization_barrier(jnp.sum(jnp.exp(capped_reference), axis=1)))
    mixture_total = jnp.log(lax.optimization_barrier(jnp.sum(jnp.exp(mixed), axis=1)))
    mixture_shift = mixed - mixture_total[:, None] - (capped_policy - policy_total[:, None])
    chosen = sampled_tokens.astype(jnp.int32)[:, None]
    policy_pick = jnp.take_along_axis(capped_policy, chosen, axis=1)[:, 0]
    reference_pick = jnp.take_along_axis(capped_reference, chosen, axis=1)[:, 0]
    mixed_pick = (1.0 - mixture_weight) * policy_pick + mixture_weight * reference_pick
    sampled_logprobs = jnp.stack([policy_pick - policy_total, reference_pick - reference_total, mixed_pick - mixture_total])
    return (mixture_shift, sampled_logprobs)
```

```python
import functools

import jax
import jax.numpy as jnp
from jax import lax
from jax.experimental import pallas as pl
from jax.experimental.pallas import tpu as pltpu
from jax.sharding import PartitionSpec as P

softcap = 30.0
epsilon = 1e-06
LANES = 128
LOG2E = 1.4426950408889634
TILE = 512
SLOT_BYTES = 40 * 2**20
ROWS = 32
POLICY_PARTS = (2, 4, 4, 4)
REFERENCE_PARTS = (7, 7)
MESH = pl.DeviceIdType.MESH


def lane_sum(x):
    total = x[:, :LANES]
    for k in range(1, x.shape[1] // LANES):
        total = total + x[:, k * LANES : (k + 1) * LANES]
    return total


def spread(row, lanes):
    return jnp.transpose(jnp.broadcast_to(row, (LANES, row.shape[1])))[:, :lanes]


def kernel(
    n_dp,
    n_mp,
    tile,
    slots,
    chunks,
    ph_hbm,
    rh_hbm,
    pg_hbm,
    rg_hbm,
    pe_hbm,
    re_hbm,
    weight_ref,
    token_ref,
    diff,
    delta_ref,
    logp_ref,
    hidden,
    policy_gain,
    reference_gain,
    normed,
    emb,
    accum,
    sums,
    weight_col,
    token_col,
    part_mp,
    part_dp,
    in_sem,
    emb_sem,
    send_sem,
    recv_sem,
    fsend_sem,
    frecv_sem,
    psend_sem,
    precv_sem,
    msend_sem,
    mrecv_sem,
    dsend_sem,
    drecv_sem,
):
    dp = lax.axis_index("dp")
    mp = lax.axis_index("mp")
    seq = hidden.shape[1]
    blocks = seq // 16
    group = 2 * blocks
    me = lax.rem(mp, group)
    base = mp - me
    half = lax.rem(me, 2)
    twin = me + 1 - 2 * half
    hops = range(2, group, 2)
    batch = normed.shape[1]
    vocab = pe_hbm.shape[0]
    tiles = vocab // tile
    models = range(2)
    steps = [(model, c) for model in models for c in range(len(chunks[model]))]
    gains = (policy_gain, reference_gain)

    own = pl.multiple_of(me // 2 * 16, 16)
    sources = ((ph_hbm, pg_hbm), (rh_hbm, rg_hbm))
    loads = []
    for model, (states, gain) in enumerate(sources):
        loads.append(pltpu.make_async_copy(states, hidden.at[model], in_sem.at[model, 0]))
        loads.append(pltpu.make_async_copy(gain, gains[model], in_sem.at[model, 1]))
    for load in loads:
        load.start()

    def fetch(source, t, slot):
        return pltpu.make_async_copy(
            source.at[pl.ds(t * tile, tile)], emb.at[slot], emb_sem.at[slot]
        )

    for g in range(slots):
        fetch(pe_hbm if g < tiles else re_hbm, g % tiles, g).start(priority=1)

    barrier = pltpu.get_barrier_semaphore()
    for o in range(1, n_dp):
        pl.semaphore_signal(
            barrier, inc=1, device_id={"dp": lax.rem(dp + o, n_dp)}, device_id_type=MESH
        )
    for o in range(1, n_mp):
        pl.semaphore_signal(
            barrier, inc=1, device_id={"mp": lax.rem(mp + o, n_mp)}, device_id_type=MESH
        )

    def normalize(model, row):
        row = pl.multiple_of(row, 16)
        values = hidden[model, pl.ds(row, 16)].astype(jnp.float32)
        meansq = jnp.mean(values * values, axis=-1, keepdims=True)
        gain = gains[model][...].reshape(1, values.shape[1])
        result = (values * lax.rsqrt(meansq + epsilon) * gain).astype(jnp.bfloat16)
        normed[model, pl.ds(pl.multiple_of(dp * seq + row, 16), 16)] = result

    def block(model, c, owner, member):
        start, width = chunks[model][c]
        row = pl.multiple_of(owner * seq + member // 2 * 16, 16)
        column = pl.multiple_of(start + lax.rem(member, 2) * (width // 2), 128)
        return normed.at[model, pl.ds(row, 16), pl.ds(column, width // 2)]

    offsets = sorted(range(1, n_dp), key=lambda o: min(o, n_dp - o))

    def owner_of(o):
        return lax.rem(dp + n_dp - o, n_dp)

    def gather_copy(model, c, o, owner):
        return pltpu.make_async_remote_copy(
            src_ref=block(model, c, owner, me),
            dst_ref=block(model, c, owner, me),
            send_sem=send_sem.at[model, c, o],
            recv_sem=recv_sem.at[model, c, o],
            device_id={"dp": lax.rem(dp + o, n_dp)},
            device_id_type=MESH,
        )

    def member_of(index, q):
        return lax.rem(index + group - q, group)

    def pass_on(model, c, o, q, member):
        return pltpu.make_async_remote_copy(
            src_ref=block(model, c, owner_of(o), member),
            dst_ref=block(model, c, owner_of(o), member),
            send_sem=psend_sem.at[model, c, o, q // 2],
            recv_sem=precv_sem.at[model, c, o, q // 2],
            device_id={"mp": base + lax.rem(me + q, group)},
            device_id_type=MESH,
        )

    def forward(model, c, o, q, member):
        return pltpu.make_async_remote_copy(
            src_ref=block(model, c, owner_of(o), member),
            dst_ref=block(model, c, owner_of(o), member),
            send_sem=fsend_sem.at[model, c, o, q // 2],
            recv_sem=frecv_sem.at[model, c, o, q // 2],
            device_id={"mp": base + twin},
            device_id_type=MESH,
        )

    def stage_a(model, c):
        for o in offsets:
            gather_copy(model, c, o, owner_of(o)).wait_recv()
            for q in hops:
                pass_on(model, c, o, q, me).start()
            forward(model, c, o, 0, me).start()

    def stage_b(model, c):
        for o in offsets:
            for q in hops:
                member = member_of(me, q)
                pass_on(model, c, o, q, member).wait_recv()
                forward(model, c, o, q, member).start()

    def stage_c(model, c):
        for o in offsets:
            for q in range(0, group, 2):
                forward(model, c, o, q, member_of(twin, q)).wait_recv()

    with jax.named_scope("p01_load"):
        loads[0].wait()
        loads[1].wait()
    normalize(0, own)
    with jax.named_scope("p02_barrier"):
        pl.semaphore_wait(barrier, n_dp - 1 + n_mp - 1)
    for c in range(len(chunks[0])):
        for o in offsets:
            gather_copy(0, c, o, dp).start()
    loads[2].wait()
    loads[3].wait()
    normalize(1, own)
    for c in range(len(chunks[1])):
        for o in offsets:
            gather_copy(1, c, o, dp).start()
    with jax.named_scope("p03_norm"):
        for model in models:
            for b in range(1, blocks):
                normalize(model, lax.rem(me // 2 + b, blocks) * 16)

    first = (dp * n_mp + mp) * vocab
    weight = weight_ref[...]
    weight_col[...] = spread(weight, LANES)
    local_token = token_ref[...] - first
    token_col[...] = spread(local_token, LANES)
    sums[...] = jnp.zeros_like(sums)

    def dot(model, c, slot, span):
        start, width = span
        return lax.dot_general(
            normed[model, :, start : start + width],
            emb[slot, :, start : start + width],
            (((1,), (1,)), ((), ())),
            preferred_element_type=jnp.float32,
        )

    def cap(raw):
        return jnp.tanh(raw * (1.0 / softcap))

    def exp_of(share):
        return jnp.exp2(share * (softcap * LOG2E))

    def columns(t):
        return pl.ds(t * tile, tile)

    def arrive(model, t):
        g = model * tiles + t
        fetch(re_hbm if model else pe_hbm, t, g % slots).wait()

    def refill(model, t):
        g = model * tiles + t
        later = g + slots
        if later < 2 * tiles:
            fetch(pe_hbm if later < tiles else re_hbm, later % tiles, g % slots).start(priority=1)

    def policy_end(t, raw):
        capped = cap(raw)
        diff[:, columns(t)] = capped
        sums[0] += lane_sum(exp_of(capped))

    def reference_end(t, raw):
        capped = cap(raw)
        policy = diff[:, columns(t)]
        w = jnp.concatenate([weight_col[...]] * (tile // LANES), axis=1)
        moved = w * (capped - policy)
        diff[:, columns(t)] = moved
        sums[1] += lane_sum(exp_of(capped))
        sums[2] += lane_sum(exp_of(policy + moved))
        lane = lax.broadcasted_iota(jnp.int32, (batch, LANES), 1)
        token = token_col[...] - (t * tile)
        policy_pick = sums[3]
        reference_pick = sums[4]
        for k in range(tile // LANES):
            hit = token == lane + k * LANES
            part = slice(k * LANES, (k + 1) * LANES)
            policy_pick = jnp.where(hit, policy[:, part], policy_pick)
            reference_pick = jnp.where(hit, capped[:, part], reference_pick)
        sums[3] = policy_pick
        sums[4] = reference_pick

    ends = (policy_end, reference_end)
    totals = (diff, accum)

    def compute(model, c, low, high):
        last = c == len(chunks[model]) - 1
        total = totals[model]
        spans = range(low, high)
        if c == 0:
            for t in spans:
                arrive(model, t)
        for t in spans:
            raw = dot(model, c, (model * tiles + t) % slots, chunks[model][c])
            if c > 0:
                raw = total[:, columns(t)] + raw
            if last:
                ends[model](t, raw)
            else:
                total[:, columns(t)] = raw
        if last:
            for t in spans:
                refill(model, t)

    count = len(steps)
    middle = tiles // 2

    def stage(run, index):
        if index < count:
            run(*steps[index])

    with jax.named_scope("p04_first"):
        stage(stage_a, 0)
        stage(stage_a, 1)
        stage(stage_a, 2)
        stage(stage_b, 0)
        stage(stage_c, 0)
    for index, (model, c) in enumerate(steps):
        if middle:
            with jax.named_scope(f"p1{index}_compute_a"):
                compute(model, c, 0, middle)
        if index:
            with jax.named_scope(f"p1{index}_service_b"):
                stage(stage_a, index + 3)
                stage(stage_b, index + 1)
        with jax.named_scope(f"p1{index}_compute_c"):
            compute(model, c, middle, tiles)
        with jax.named_scope(f"p1{index}_service_d"):
            if index == 0:
                stage(stage_a, 3)
                stage(stage_b, 1)
            stage(stage_c, index + 1)

    lane = lax.broadcasted_iota(jnp.int32, (batch, LANES), 1)
    packed = jnp.zeros((batch, LANES), jnp.float32)
    for k in range(5):
        scale = 1.0 if k < 3 else softcap
        packed = jnp.where(lane == k, jnp.sum(sums[k], axis=1, keepdims=True) * scale, packed)
    part_mp[0] = jnp.transpose(packed)[:8]

    def share(buffer, axis, me, n, o, send, recv):
        return pltpu.make_async_remote_copy(
            src_ref=buffer.at[0],
            dst_ref=buffer.at[o],
            send_sem=send.at[o],
            recv_sem=recv.at[o],
            device_id={axis: lax.rem(me + o, n)},
            device_id_type=MESH,
        )

    def begin(buffer, axis, me, n, send, recv):
        for o in range(1, n):
            share(buffer, axis, me, n, o, send, recv).start()

    def finish(buffer, axis, me, n, send, recv):
        for o in range(1, n):
            share(buffer, axis, me, n, o, send, recv).wait_recv()
        total = buffer[0]
        for o in range(1, n):
            total = total + buffer[o]
        return total

    begin(part_mp, "mp", mp, n_mp, msend_sem, mrecv_sem)
    with jax.named_scope("p90_waitsend"):
        for model, c in steps:
            for o in offsets:
                gather_copy(model, c, o, dp).wait_send()
                for q in hops:
                    pass_on(model, c, o, q, me).wait_send()
                for q in range(0, group, 2):
                    forward(model, c, o, q, member_of(me, q)).wait_send()
    with jax.named_scope("p91_redmp"):
        part_dp[0] = finish(part_mp, "mp", mp, n_mp, msend_sem, mrecv_sem)
    begin(part_dp, "dp", dp, n_dp, dsend_sem, drecv_sem)
    for o in range(1, n_mp):
        share(part_mp, "mp", mp, n_mp, o, msend_sem, mrecv_sem).wait_send()
    with jax.named_scope("p92_reddp"):
        total = finish(part_dp, "dp", dp, n_dp, dsend_sem, drecv_sem)
    policy_total = jnp.log(total[0:1])
    reference_total = jnp.log(total[1:2])
    mixture_total = jnp.log(total[2:3])
    policy_pick = total[3:4]
    reference_pick = total[4:5]
    mixed_pick = (1.0 - weight) * policy_pick + weight * reference_pick
    logp = (policy_pick - policy_total, reference_pick - reference_total, mixed_pick - mixture_total)
    for k, row in enumerate(logp):
        mine = row[:, :seq]
        for owner in range(1, n_dp):
            mine = jnp.where(dp == owner, row[:, owner * seq : (owner + 1) * seq], mine)
        logp_ref[k : k + 1] = mine
    delta_ref[...] = spread(mixture_total - policy_total, LANES)
    for o in range(1, n_dp):
        share(part_dp, "dp", dp, n_dp, o, dsend_sem, drecv_sem).wait_send()


def finish_kernel(rows, diff, delta, logp, out_hbm, logp_out, staged, sem):
    copies = []
    for b in range(diff.shape[0] // rows):
        part = slice(b * rows, (b + 1) * rows)
        shift = delta[part, :]
        for k in range(diff.shape[1] // LANES):
            lanes = slice(k * LANES, (k + 1) * LANES)
            staged[part, lanes] = diff[part, lanes] * softcap - shift
        copy = pltpu.make_async_copy(staged.at[part], out_hbm.at[part], sem.at[b])
        copy.start()
        copies.append(copy)
    logp_out[...] = logp[...]
    for copy in copies:
        copy.wait()


def split(width, parts):
    unit = width // sum(parts)
    spans, start = [], 0
    for part in parts:
        spans.append((start, part * unit))
        start += part * unit
    return tuple(spans)


def local(
    n_dp,
    n_mp,
    policy_hidden,
    reference_hidden,
    policy_gain,
    reference_gain,
    policy_embedding,
    reference_embedding,
    mixture_weight,
    sampled_tokens,
):
    seq, width = policy_hidden.shape
    vocab = policy_embedding.shape[0]
    batch = mixture_weight.shape[0]
    tile = min(TILE, vocab)
    tiles = vocab // tile
    slots = min(2 * tiles, SLOT_BYTES // (tile * width * 2))
    assert slots >= tiles
    half = seq // 16
    parts = POLICY_PARTS, REFERENCE_PARTS
    if n_dp > 4:
        parts = (1,), (1,)
    chunks = tuple(split(width, p) for p in parts)
    count = max(len(c) for c in chunks)
    anywhere = pl.BlockSpec(memory_space=pl.ANY)
    vmem = pl.BlockSpec(memory_space=pltpu.VMEM)
    dma = pltpu.SemaphoreType.DMA
    diff, delta, logp = pl.pallas_call(
        functools.partial(kernel, n_dp, n_mp, tile, slots, chunks),
        name="mixture",
        out_shape=(
            pltpu.VMEM((batch, vocab), jnp.float32),
            pltpu.VMEM((batch, LANES), jnp.float32),
            pltpu.VMEM((3, seq), jnp.float32),
        ),
        in_specs=[anywhere] * 6 + [vmem] * 2,
        out_specs=(vmem, vmem, vmem),
        scratch_shapes=[
            pltpu.VMEM((2, seq, width), jnp.bfloat16),
            pltpu.VMEM((width,), jnp.float32),
            pltpu.VMEM((width,), jnp.float32),
            pltpu.VMEM((2, batch, width), jnp.bfloat16),
            pltpu.VMEM((slots, tile, width), jnp.bfloat16),
            pltpu.VMEM((batch, vocab), jnp.float32),
            pltpu.VMEM((5, batch, LANES), jnp.float32),
            pltpu.VMEM((batch, LANES), jnp.float32),
            pltpu.VMEM((batch, LANES), jnp.int32),
            pltpu.VMEM((n_mp, 8, batch), jnp.float32),
            pltpu.VMEM((n_dp, 8, batch), jnp.float32),
            dma((2, 2)),
            dma((slots,)),
            dma((2, count, n_dp)),
            dma((2, count, n_dp)),
            dma((2, count, n_dp, half)),
            dma((2, count, n_dp, half)),
            dma((2, count, n_dp, half)),
            dma((2, count, n_dp, half)),
            dma((n_mp,)),
            dma((n_mp,)),
            dma((n_dp,)),
            dma((n_dp,)),
        ],
        compiler_params=pltpu.CompilerParams(
            collective_id=0, has_side_effects=True, vmem_limit_bytes=54 * 2**20
        ),
    )(
        policy_hidden,
        reference_hidden,
        policy_gain,
        reference_gain,
        policy_embedding,
        reference_embedding,
        mixture_weight.reshape(1, batch),
        sampled_tokens.reshape(1, batch),
    )
    return tuple(
        pl.pallas_call(
            functools.partial(finish_kernel, ROWS),
            name="shift",
            out_shape=(
                jax.ShapeDtypeStruct((batch, vocab), jnp.float32),
                jax.ShapeDtypeStruct((3, seq), jnp.float32),
            ),
            in_specs=[vmem] * 3,
            out_specs=(anywhere, vmem),
            scratch_shapes=[pltpu.VMEM((batch, vocab), jnp.float32), dma((batch // ROWS,))],
            compiler_params=pltpu.CompilerParams(vmem_limit_bytes=12 * 2**20),
        )(*(pltpu.with_memory_space_constraint(x, pltpu.VMEM) for x in (diff, delta, logp)))
    )


def solution(mesh):
    in_specs = (
        P("dp", None),
        P("dp", None),
        P(),
        P(),
        P(("dp", "mp"), None),
        P(("dp", "mp"), None),
        P(),
        P(),
    )
    out_specs = (P(None, ("dp", "mp")), P(None, "dp"))
    body = functools.partial(local, mesh.shape["dp"], mesh.shape["mp"])
    return jax.shard_map(body, mesh=mesh, in_specs=in_specs, out_specs=out_specs, check_vma=False)
```

```python
import functools

import jax
import jax.numpy as jnp
from jax import lax
from jax.experimental import pallas as pl
from jax.experimental.pallas import tpu as pltpu
from jax.sharding import PartitionSpec as P

softcap = 30.0
epsilon = 1e-06
LANES = 128
LOG2E = 1.4426950408889634
TILE = 512
SLOT_BYTES = 43 * 2**20
ROWS = 32
BLOCK = 16
POLICY_PARTS = (2, 4, 4, 4)
REFERENCE_PARTS = (5, 9)
CUTS = (6, 8)
MESH = pl.DeviceIdType.MESH


def lane_sum(x):
    total = x[:, :LANES]
    for k in range(1, x.shape[1] // LANES):
        total = total + x[:, k * LANES : (k + 1) * LANES]
    return total


def spread(row, lanes):
    return jnp.transpose(jnp.broadcast_to(row, (LANES, row.shape[1])))[:, :lanes]


def kernel(
    n_dp,
    n_mp,
    tile,
    slots,
    chunks,
    cuts,
    ph_hbm,
    rh_hbm,
    pg_hbm,
    rg_hbm,
    pe_hbm,
    re_hbm,
    weight_ref,
    token_ref,
    diff,
    delta_ref,
    logp_ref,
    hidden,
    policy_gain,
    reference_gain,
    normed,
    emb,
    accum,
    sums,
    weight_col,
    token_col,
    part_mp,
    part_dp,
    in_sem,
    emb_sem,
    send_sem,
    recv_sem,
    fsend_sem,
    frecv_sem,
    psend_sem,
    precv_sem,
    msend_sem,
    mrecv_sem,
    dsend_sem,
    drecv_sem,
):
    dp = lax.axis_index("dp")
    mp = lax.axis_index("mp")
    seq, width = hidden.shape[1:]
    blocks = seq // 16
    group = 2 * blocks
    me = lax.rem(mp, group)
    base = mp - me
    half = lax.rem(me, 2)
    twin = me + 1 - 2 * half
    hops = range(2, group, 2)
    batch = normed.shape[1]
    vocab = pe_hbm.shape[0]
    tiles = vocab // tile
    models = range(2)
    steps = [(model, c) for model in models for c in range(len(chunks[model]))]
    gains = (policy_gain, reference_gain)

    own = pl.multiple_of(me // 2 * 16, 16)
    sources = ((ph_hbm, pg_hbm), (rh_hbm, rg_hbm))
    loads = []
    for model, (states, gain) in enumerate(sources):
        loads.append(pltpu.make_async_copy(states, hidden.at[model], in_sem.at[model, 0]))
        loads.append(pltpu.make_async_copy(gain, gains[model], in_sem.at[model, 1]))
    for load in loads:
        load.start()

    def fetch(g, piece):
        source = re_hbm if g // tiles else pe_hbm
        start, span = cuts[piece]
        return pltpu.make_async_copy(
            source.at[pl.ds(g % tiles * tile, tile), pl.ds(start, span)],
            emb.at[g % slots, :, pl.ds(start, span)],
            emb_sem.at[g % slots, piece],
        )

    for held in (range(tiles), range(tiles, slots)):
        for piece in range(len(cuts)):
            for g in held:
                fetch(g, piece).start(priority=1)

    barrier = pltpu.get_barrier_semaphore()
    for o in range(1, n_dp):
        pl.semaphore_signal(
            barrier, inc=1, device_id={"dp": lax.rem(dp + o, n_dp)}, device_id_type=MESH
        )
    for o in range(1, n_mp):
        pl.semaphore_signal(
            barrier, inc=1, device_id={"mp": lax.rem(mp + o, n_mp)}, device_id_type=MESH
        )

    def normalize(model, row):
        row = pl.multiple_of(row, 16)
        values = hidden[model, pl.ds(row, 16)].astype(jnp.float32)
        meansq = jnp.mean(values * values, axis=-1, keepdims=True)
        gain = gains[model][...].reshape(1, values.shape[1])
        result = (values * lax.rsqrt(meansq + epsilon) * gain).astype(jnp.bfloat16)
        normed[model, pl.ds(pl.multiple_of(dp * seq + row, 16), 16)] = result

    def block(model, c, owner, member):
        start, span = chunks[model][c]
        row = pl.multiple_of(owner * seq + member // 2 * 16, 16)
        column = pl.multiple_of(start + lax.rem(member, 2) * (span // 2), 128)
        return normed.at[model, pl.ds(row, 16), pl.ds(column, span // 2)]

    offsets = sorted(range(1, n_dp), key=lambda o: min(o, n_dp - o))

    def owner_of(o):
        return lax.rem(dp + n_dp - o, n_dp)

    order = {step: index for index, step in enumerate(steps)}

    def gather_copy(model, c, o, owner):
        return pltpu.make_async_remote_copy(
            src_ref=block(model, c, owner, me),
            dst_ref=block(model, c, owner, me),
            send_sem=send_sem.at[model],
            recv_sem=recv_sem.at[order[model, c], o - 1],
            device_id={"dp": lax.rem(dp + o, n_dp)},
            device_id_type=MESH,
        )

    def member_of(index, q):
        return lax.rem(index + group - q, group)

    def pass_on(model, c, o, q, member):
        return pltpu.make_async_remote_copy(
            src_ref=block(model, c, owner_of(o), member),
            dst_ref=block(model, c, owner_of(o), member),
            send_sem=psend_sem.at[model],
            recv_sem=precv_sem.at[order[model, c]],
            device_id={"mp": base + lax.rem(me + q, group)},
            device_id_type=MESH,
        )

    def forward(model, c, o, q, member):
        return pltpu.make_async_remote_copy(
            src_ref=block(model, c, owner_of(o), member),
            dst_ref=block(model, c, owner_of(o), member),
            send_sem=fsend_sem.at[model],
            recv_sem=frecv_sem.at[order[model, c]],
            device_id={"mp": base + twin},
            device_id_type=MESH,
        )

    def drain(model, columns, count, sem):
        view = normed.at[model, pl.ds(0, 16 * count), pl.ds(0, columns // 2)]
        pltpu.make_async_copy(view, view, sem).wait()

    peers = n_dp - 1

    def stage_a(model, c):
        for o in offsets:
            gather_copy(model, c, o, owner_of(o)).wait_recv()
            for q in hops:
                pass_on(model, c, o, q, me).start()
            forward(model, c, o, 0, me).start()

    def stage_b(model, c):
        drain(model, chunks[model][c][1], peers * (blocks - 1), precv_sem.at[order[model, c]])
        for o in offsets:
            for q in hops:
                forward(model, c, o, q, member_of(me, q)).start()

    def stage_c(model, c):
        drain(model, chunks[model][c][1], peers * blocks, frecv_sem.at[order[model, c]])

    with jax.named_scope("p01_load"):
        loads[0].wait()
        loads[1].wait()
    normalize(0, own)
    with jax.named_scope("p02_barrier"):
        pl.semaphore_wait(barrier, n_dp - 1 + n_mp - 1)
    for c in range(len(chunks[0])):
        for o in offsets:
            gather_copy(0, c, o, dp).start()
    loads[2].wait()
    loads[3].wait()
    normalize(1, own)
    for c in range(len(chunks[1])):
        for o in offsets:
            gather_copy(1, c, o, dp).start()
    with jax.named_scope("p03_norm"):
        for model in models:
            for b in range(1, blocks):
                normalize(model, lax.rem(me // 2 + b, blocks) * 16)

    first = (dp * n_mp + mp) * vocab
    weight = weight_ref[...]
    weight_col[...] = spread(weight, LANES)
    local_token = token_ref[...] - first
    token_col[...] = spread(local_token, LANES)
    sums[...] = jnp.zeros_like(sums)

    def dot(model, c, slot, span):
        part = slice(span[0], sum(span))
        return lax.dot_general(
            normed[model, :, part],
            emb[slot, :, part],
            (((1,), (1,)), ((), ())),
            preferred_element_type=jnp.float32,
        )

    def cap(raw):
        return jnp.tanh(raw * (1.0 / softcap))

    def exp_of(share):
        return jnp.exp2(share * (softcap * LOG2E))

    def columns(t):
        return pl.ds(t * tile, tile)

    def arrive(model, c, t):
        for piece, (start, span) in enumerate(cuts):
            if chunks[model][c][0] <= start < sum(chunks[model][c]):
                fetch(model * tiles + t, piece).wait()

    def refill(model, c, t):
        later = model * tiles + t + slots
        for piece, (start, span) in enumerate(cuts):
            if chunks[model][c][0] < start + span <= sum(chunks[model][c]) and later < 2 * tiles:
                fetch(later, piece).start(priority=1)

    def policy_end(t):
        for r in range(0, batch, BLOCK):
            rows = pl.ds(r, BLOCK)
            capped = cap(diff[rows, columns(t)])
            diff[rows, columns(t)] = capped
            sums[0, rows] += lane_sum(exp_of(capped))

    def reference_end(t):
        lane = lax.broadcasted_iota(jnp.int32, (BLOCK, tile), 1) + t * tile
        for r in range(0, batch, BLOCK):
            rows = pl.ds(r, BLOCK)
            capped = cap(accum[rows, columns(t)])
            policy = diff[rows, columns(t)]
            w = jnp.concatenate([weight_col[rows]] * (tile // LANES), axis=1)
            moved = w * (capped - policy)
            diff[rows, columns(t)] = moved
            sums[1, rows] += lane_sum(exp_of(capped))
            sums[2, rows] += lane_sum(exp_of(policy + moved))
            token = token_col[rows]
            policy_pick = sums[3, rows]
            reference_pick = sums[4, rows]
            for k in range(tile // LANES):
                part = slice(k * LANES, (k + 1) * LANES)
                hit = token == lane[:, part]
                policy_pick = jnp.where(hit, policy[:, part], policy_pick)
                reference_pick = jnp.where(hit, capped[:, part], reference_pick)
            sums[3, rows] = policy_pick
            sums[4, rows] = reference_pick

    ends = (policy_end, reference_end)
    totals = (diff, accum)

    pending = []

    def flush():
        while pending:
            model, t = pending.pop()
            ends[model](t)

    def compute(model, c, low, high):
        last = c == len(chunks[model]) - 1
        total = totals[model]
        for t in range(low, high):
            raw = dot(model, c, (model * tiles + t) % slots, chunks[model][c])
            if c > 0:
                raw = total[:, columns(t)] + raw
            total[:, columns(t)] = raw
            flush()
            if last:
                pending.append((model, t))
        for t in range(low, high):
            refill(model, c, t)

    count = len(steps)
    middle = tiles // 2

    def stage(run, index):
        if index < count:
            run(*steps[index])

    with jax.named_scope("p04_first"):
        stage(stage_a, 0)
        stage(stage_a, 1)
        stage(stage_b, 0)
        stage(stage_a, 2)
        stage(stage_c, 0)
    for index, (model, c) in enumerate(steps):
        for t in range(tiles):
            arrive(model, c, t)
        if middle:
            with jax.named_scope(f"p1{index}_compute_a"):
                compute(model, c, 0, middle)
        with jax.named_scope(f"p1{index}_service_b"):
            if index == 0:
                stage(stage_a, 3)
            stage(stage_b, index + 1)
        with jax.named_scope(f"p1{index}_compute_c"):
            compute(model, c, middle, tiles)
        with jax.named_scope(f"p1{index}_service_d"):
            stage(stage_c, index + 1)
            stage(stage_a, index + 4)
    flush()

    lane = lax.broadcasted_iota(jnp.int32, (batch, LANES), 1)
    packed = jnp.zeros((batch, LANES), jnp.float32)
    for k in range(5):
        scale = 1.0 if k < 3 else softcap
        packed = jnp.where(lane == k, jnp.sum(sums[k], axis=1, keepdims=True) * scale, packed)
    part_mp[0] = jnp.transpose(packed)[:8]

    def share(buffer, axis, me, n, o, send, recv):
        return pltpu.make_async_remote_copy(
            src_ref=buffer.at[0],
            dst_ref=buffer.at[o],
            send_sem=send.at[0],
            recv_sem=recv.at[0],
            device_id={axis: lax.rem(me + o, n)},
            device_id_type=MESH,
        )

    def settle(buffer, n, sem):
        view = buffer.at[pl.ds(1, n - 1)]
        pltpu.make_async_copy(view, view, sem.at[0]).wait()

    def begin(buffer, axis, me, n, send, recv):
        for o in range(1, n):
            share(buffer, axis, me, n, o, send, recv).start()

    def finish(buffer, n, recv):
        settle(buffer, n, recv)
        total = buffer[0]
        for o in range(1, n):
            total = total + buffer[o]
        return total

    begin(part_mp, "mp", mp, n_mp, msend_sem, mrecv_sem)
    with jax.named_scope("p90_waitsend"):
        for model in models:
            drain(model, width, peers, send_sem.at[model])
            drain(model, width, peers * (blocks - 1), psend_sem.at[model])
            drain(model, width, peers * blocks, fsend_sem.at[model])
    with jax.named_scope("p91_redmp"):
        part_dp[0] = finish(part_mp, n_mp, mrecv_sem)
    begin(part_dp, "dp", dp, n_dp, dsend_sem, drecv_sem)
    settle(part_mp, n_mp, msend_sem)
    with jax.named_scope("p92_reddp"):
        total = finish(part_dp, n_dp, drecv_sem)
    policy_total = jnp.log(total[0:1])
    reference_total = jnp.log(total[1:2])
    mixture_total = jnp.log(total[2:3])
    policy_pick = total[3:4]
    reference_pick = total[4:5]
    mixed_pick = (1.0 - weight) * policy_pick + weight * reference_pick
    logp = (policy_pick - policy_total, reference_pick - reference_total, mixed_pick - mixture_total)
    for k, row in enumerate(logp):
        mine = row[:, :seq]
        for owner in range(1, n_dp):
            mine = jnp.where(dp == owner, row[:, owner * seq : (owner + 1) * seq], mine)
        logp_ref[k : k + 1] = mine
    delta_ref[...] = spread(mixture_total - policy_total, LANES)
    settle(part_dp, n_dp, dsend_sem)


def finish_kernel(rows, diff, delta, logp, out_hbm, logp_out, staged, sem):
    copies = []
    for b in range(diff.shape[0] // rows):
        part = slice(b * rows, (b + 1) * rows)
        shift = delta[part, :]
        for k in range(diff.shape[1] // LANES):
            lanes = slice(k * LANES, (k + 1) * LANES)
            staged[part, lanes] = diff[part, lanes] * softcap - shift
        copy = pltpu.make_async_copy(staged.at[part], out_hbm.at[part], sem.at[b])
        copy.start()
        copies.append(copy)
    logp_out[...] = logp[...]
    for copy in copies:
        copy.wait()


def split(width, parts):
    unit = width // sum(parts)
    spans, start = [], 0
    for part in parts:
        spans.append((start, part * unit))
        start += part * unit
    return tuple(spans)


def local(
    n_dp,
    n_mp,
    policy_hidden,
    reference_hidden,
    policy_gain,
    reference_gain,
    policy_embedding,
    reference_embedding,
    mixture_weight,
    sampled_tokens,
):
    seq, width = policy_hidden.shape
    vocab = policy_embedding.shape[0]
    batch = mixture_weight.shape[0]
    tile = min(TILE, vocab)
    tiles = vocab // tile
    slots = min(2 * tiles, SLOT_BYTES // (tile * width * 2))
    assert slots >= tiles
    parts = POLICY_PARTS, REFERENCE_PARTS
    if n_dp > 4:
        parts = (1,), (1,)
    chunks = tuple(split(width, p) for p in parts)
    count = sum(len(c) for c in chunks)
    cuts = split(width, CUTS if n_dp <= 4 else (1,))
    anywhere = pl.BlockSpec(memory_space=pl.ANY)
    vmem = pl.BlockSpec(memory_space=pltpu.VMEM)
    dma = pltpu.SemaphoreType.DMA
    diff, delta, logp = pl.pallas_call(
        functools.partial(kernel, n_dp, n_mp, tile, slots, chunks, cuts),
        name="mixture",
        out_shape=(
            pltpu.VMEM((batch, vocab), jnp.float32),
            pltpu.VMEM((batch, LANES), jnp.float32),
            pltpu.VMEM((3, seq), jnp.float32),
        ),
        in_specs=[anywhere] * 6 + [vmem] * 2,
        out_specs=(vmem, vmem, vmem),
        scratch_shapes=[
            pltpu.VMEM((2, seq, width), jnp.bfloat16),
            pltpu.VMEM((width,), jnp.float32),
            pltpu.VMEM((width,), jnp.float32),
            pltpu.VMEM((2, batch, width), jnp.bfloat16),
            pltpu.VMEM((slots, tile, width), jnp.bfloat16),
            pltpu.VMEM((batch, vocab), jnp.float32),
            pltpu.VMEM((5, batch, LANES), jnp.float32),
            pltpu.VMEM((batch, LANES), jnp.float32),
            pltpu.VMEM((batch, LANES), jnp.int32),
            pltpu.VMEM((n_mp, 8, batch), jnp.float32),
            pltpu.VMEM((n_dp, 8, batch), jnp.float32),
            dma((2, 2)),
            dma((slots, len(cuts))),
            dma((2,)),
            dma((count, n_dp - 1)),
            dma((2,)),
            dma((count,)),
            dma((2,)),
            dma((count,)),
            dma((1,)),
            dma((1,)),
            dma((1,)),
            dma((1,)),
        ],
        compiler_params=pltpu.CompilerParams(
            collective_id=0, has_side_effects=True, vmem_limit_bytes=54 * 2**20
        ),
    )(
        policy_hidden,
        reference_hidden,
        policy_gain,
        reference_gain,
        policy_embedding,
        reference_embedding,
        mixture_weight.reshape(1, batch),
        sampled_tokens.reshape(1, batch),
    )
    return tuple(
        pl.pallas_call(
            functools.partial(finish_kernel, ROWS),
            name="shift",
            out_shape=(
                jax.ShapeDtypeStruct((batch, vocab), jnp.float32),
                jax.ShapeDtypeStruct((3, seq), jnp.float32),
            ),
            in_specs=[vmem] * 3,
            out_specs=(anywhere, vmem),
            scratch_shapes=[pltpu.VMEM((batch, vocab), jnp.float32), dma((batch // ROWS,))],
            compiler_params=pltpu.CompilerParams(vmem_limit_bytes=12 * 2**20),
        )(*(pltpu.with_memory_space_constraint(x, pltpu.VMEM) for x in (diff, delta, logp)))
    )


def solution(mesh):
    in_specs = (
        P("dp", None),
        P("dp", None),
        P(),
        P(),
        P(("dp", "mp"), None),
        P(("dp", "mp"), None),
        P(),
        P(),
    )
    out_specs = (P(None, ("dp", "mp")), P(None, "dp"))
    body = functools.partial(local, mesh.shape["dp"], mesh.shape["mp"])
    return jax.shard_map(body, mesh=mesh, in_specs=in_specs, out_specs=out_specs, check_vma=False)
```
